16 devices in a mesh: dp: 1, tp: 16 (over x, y, z, core).
Axes of the slice: x: 2, y: 2, z: 2, core: 2. Of those that a mesh axis runs over, the one named last changes fastest.
Arguments:
- x: bfloat16 [64, 3072], P('dp')
- k_cache: bfloat16 [64, 4096, 32, 96], P('dp', None, 'tp')
- v_cache: bfloat16 [64, 4096, 32, 96], P('dp', None, 'tp')
- gain_a: bfloat16 [3072], replicated
- wq: bfloat16 [3072, 3072], P(None, 'tp')
- wo: bfloat16 [3072, 3072], P('tp')
- gain_m: bfloat16 [3072], replicated
- w_gate: bfloat16 [3072, 8192], P(None, 'tp')
- w_up: bfloat16 [3072, 8192], P(None, 'tp')
- w_down: bfloat16 [8192, 3072], P('tp')
Outputs:
- output: bfloat16 [64, 3072], P('dp')
All inputs are finite; a program needn't handle non-finite values.
Results may differ from the reference program's by a relative error of at most 0.017.
Values are sent between devices in bfloat16 or wider.
A program may use at most 2 GiB of HBM per device.

```python
import jax
import jax.numpy as jnp
from jax import lax

BATCH = 64
CACHE = 4096
D = 3072
HEADS = 32
KV_HEADS = 32
HEAD = 96
FF = 8192
THETA = 10000


def setup_inputs(seed: int = 0, part: int = 0) -> dict:
    kx, kc, kw, kn, kq, ko, km, kg, ku, kd = jax.random.split(jax.random.key(seed), 10)
    kx, kc, kw = (jax.random.fold_in(k, part) for k in (kx, kc, kw))

    def weights(key, rows, columns):
        return jax.random.normal(key, (rows, columns), jnp.float32) * rows**-0.5

    drawn = {
        "x": jax.random.normal(kx, (BATCH, D), jnp.float32),
        "k_cache": 2 * jax.random.normal(kc, (BATCH, CACHE, KV_HEADS, HEAD), jnp.float32),
        "v_cache": 4 * jax.random.normal(kw, (BATCH, CACHE, KV_HEADS, HEAD), jnp.float32),
        "gain_a": 1 + 0.1 * jax.random.normal(kn, (D,), jnp.float32),
        "wq": 2 * weights(kq, D, HEADS * HEAD),
        "wo": weights(ko, HEADS * HEAD, D),
        "gain_m": 1 + 0.1 * jax.random.normal(km, (D,), jnp.float32),
        "w_gate": weights(kg, D, FF),
        "w_up": weights(ku, D, FF),
        "w_down": 2 * weights(kd, FF, D),
    }
    return {k: v.astype(jnp.bfloat16) for k, v in drawn.items()}


def normed(x, gain):
    wide = x.astype(jnp.float32)
    scale = lax.rsqrt(jnp.mean(wide * wide, -1, keepdims=True) + 1e-6)
    return (wide * scale * gain.astype(jnp.float32)).astype(jnp.bfloat16)


def turned(t, place, theta):
    half = t.shape[-1] // 2
    angle = place.astype(jnp.float32)[:, None] * theta ** (-jnp.arange(half, dtype=jnp.float32) / half)
    cos, sin = jnp.cos(angle)[:, None], jnp.sin(angle)[:, None]
    a, b = t[..., :half].astype(jnp.float32), t[..., half:].astype(jnp.float32)
    return jnp.concatenate([a * cos - b * sin, b * cos + a * sin], -1).astype(jnp.bfloat16)


def matmul(a, w):
    return jnp.dot(a, w, preferred_element_type=jnp.float32).astype(jnp.bfloat16)


def einsum(form, a, b):
    return jnp.einsum(form, a.astype(jnp.float32), b.astype(jnp.float32))


def seen_by(a, wq, k_cache, v_cache, head, theta):
    batch, cache, kv_heads = k_cache.shape[:3]
    place = jnp.full((batch,), cache - 1)
    q = turned(matmul(a, wq).reshape(batch, -1, head), place, theta).reshape(batch, kv_heads, -1, head)
    scores = einsum("bgsd,bugd->bgsu", q, k_cache) * head**-0.5
    weights = jax.nn.softmax(scores, -1).astype(jnp.bfloat16)
    return einsum("bgsu,bugd->bgsd", weights, v_cache).astype(jnp.bfloat16).reshape(batch, -1)


def hidden_of(b, w_gate, w_up):
    gate = jnp.dot(b, w_gate, preferred_element_type=jnp.float32)
    up = jnp.dot(b, w_up, preferred_element_type=jnp.float32)
    return (jax.nn.silu(gate) * up).astype(jnp.bfloat16)


def reference(x, k_cache, v_cache, gain_a, wq, wo, gain_m, w_gate, w_up, w_down):
    seen = seen_by(normed(x, gain_a), wq, k_cache, v_cache, HEAD, THETA)
    h = (x.astype(jnp.float32) + jnp.dot(seen, wo, preferred_element_type=jnp.float32)).astype(jnp.bfloat16)
    hidden = hidden_of(normed(h, gain_m), w_gate, w_up)
    return (h.astype(jnp.float32) + jnp.dot(hidden, w_down, preferred_element_type=jnp.float32)).astype(jnp.bfloat16)
```

```python
import functools

import jax
import jax.numpy as jnp
import numpy as np
from jax import lax
from jax.experimental import pallas as pl
from jax.experimental.pallas import tpu as pltpu
from jax.sharding import PartitionSpec as P

HEAD = 96
THETA = 10000

ROWS = 64
D = 3072
SPAN = 4096
QD = 192
FF = 512
GROUP = 4
GROUPS = ROWS // GROUP
STACK = GROUP * QD
PIECES = 4
PIECE = SPAN // PIECES
SLOTS = 2
CHUNK = 16
CHUNKS = ROWS // CHUNK
PER = CHUNK // GROUP
N = 16
OWN = D // (N // 2)

F32, BF16 = jnp.float32, jnp.bfloat16
NT = (((1,), (1,)), ((), ()))


def dot(a, b):
    return jnp.dot(a, b, preferred_element_type=F32)


def iota(shape, axis):
    return lax.broadcasted_iota(jnp.int32, shape, axis)


def ones_where(keep):
    return jnp.where(keep, 1.0, 0.0).astype(BF16)


def scaled(wide, gain):
    scale = lax.rsqrt(jnp.mean(wide * wide, -1, keepdims=True) + 1e-6)
    return (wide * scale * gain).astype(BF16)


def any_of(d, values):
    found = d == values[0]
    for v in values[1:]:
        found = found | (d == v)
    return found


def kernel(
    x_hbm, k_hbm, v_hbm, turn_ref, gain_a_ref, wq_hbm, wo_hbm, gain_m_ref, wg_hbm, wu_hbm, wd_hbm,
    y_hbm,
    x_v, wq_v, wo_v, wg_v, wu_v, wd_v, k_v, v_v, q_v, s_v, w_v, fold_v, seen_v,
    p1, p2, r1, r2, hb, yb,
    k_sem, v_sem, w_sem, send_sem, recv_sem, out_sem,
):
    me = lax.axis_index("tp")
    my_chip, my_half = me // 2, me % 2
    my_columns = pl.ds(pl.multiple_of(my_chip * OWN, 128), OWN)

    def piece(i):
        return pl.ds(i * PIECE, PIECE)

    def k_copy(g, i):
        slot = lax.rem(g, SLOTS)
        return pltpu.make_async_copy(k_hbm.at[g, :, piece(i)], k_v.at[slot, :, piece(i)], k_sem.at[slot, i])

    def v_copy(g, i):
        slot = lax.rem(g, SLOTS)
        return pltpu.make_async_copy(v_hbm.at[g, :, piece(i)], v_v.at[slot, :, piece(i)], v_sem.at[slot, i])

    early = [pltpu.make_async_copy(x_hbm, x_v, w_sem.at[0]), pltpu.make_async_copy(wq_hbm, wq_v, w_sem.at[1])]
    late = [
        pltpu.make_async_copy(wo_hbm, wo_v, w_sem.at[2]),
        pltpu.make_async_copy(wg_hbm, wg_v, w_sem.at[3]),
        pltpu.make_async_copy(wu_hbm, wu_v, w_sem.at[4]),
        pltpu.make_async_copy(wd_hbm, wd_v, w_sem.at[5]),
    ]
    for copy in early:
        copy.start()
    for g in range(SLOTS):
        for i in range(PIECES):
            k_copy(g, i).start()
        for i in range(PIECES):
            v_copy(g, i).start()
    for copy in late:
        copy.start()

    barrier = pltpu.get_barrier_semaphore()
    for p in range(1, N):
        pl.semaphore_signal(barrier, inc=1, device_id={"tp": lax.rem(me + p, N)}, device_id_type=pl.DeviceIdType.MESH)

    for copy in early:
        copy.wait()
    a = scaled(x_v[...].reshape(ROWS, D).astype(F32), gain_a_ref[...].astype(F32))
    q = lax.dot_general(a, wq_v[...], NT, preferred_element_type=F32).astype(BF16)
    i, j = iota((QD, QD), 0), iota((QD, QD), 1)
    first = (j < 48) | ((j >= 96) & (j < 144))
    swapped = dot(q, ones_where(((i - j == 48) & first) | ((i - j == -48) & ~first)))
    q = (q.astype(F32) * turn_ref[0:1, :] + swapped * turn_ref[1:2, :]).astype(BF16)
    places = [QD * n for n in range(GROUP)]
    spread = ones_where(any_of(iota((QD, STACK), 1) - iota((QD, STACK), 0), places))
    wide = dot(q, spread).astype(BF16)
    i = iota((2 * ROWS, ROWS), 0)
    wide = dot(ones_where((i >> 3) * GROUP + (i & 3) == iota((2 * ROWS, ROWS), 1)), wide)
    r, c = iota((2 * ROWS, STACK), 0), iota((2 * ROWS, STACK), 1)
    low = (r & 3) * QD + ((r >> 2) & 1) * HEAD
    q_v[...] = jnp.where((c >= low) & (c < low + HEAD), wide, 0.0).reshape(GROUPS, 8, STACK)
    fold_v[...] = ones_where(any_of(iota((STACK, QD), 0) - iota((STACK, QD), 1), places))

    def attend(g):
        slot = lax.rem(g, SLOTS)
        queries = q_v[g].astype(BF16)
        for i in range(PIECES):
            k_copy(g, i).wait()
            s_v[:, piece(i)] = dot(queries, k_v[slot, :, piece(i)]) * HEAD**-0.5

            @pl.when(g + SLOTS < GROUPS)
            def _():
                k_copy(g + SLOTS, i).start()

        s = s_v[...]
        e = jnp.exp(s - jnp.max(s, -1, keepdims=True))
        w_v[...] = (e * (1.0 / jnp.sum(e, -1, keepdims=True))).astype(BF16)
        total = jnp.zeros((8, STACK), F32)
        for i in range(PIECES):
            v_copy(g, i).wait()
            total += lax.dot_general(w_v[:, piece(i)], v_v[slot, :, piece(i)], NT, preferred_element_type=F32)

            @pl.when(g + SLOTS < GROUPS)
            def _():
                v_copy(g + SLOTS, i).start()

        r, c = iota((8, STACK), 0), iota((8, STACK), 1)
        low = (r & 3) * QD + (r >> 2) * HEAD
        own = jnp.where((c >= low) & (c < low + HEAD), total, 0.0).astype(BF16)
        seen_v[g] = dot(own, fold_v[...])

    def scatter(phase, chunk, parts, landing):
        @pl.loop(1, N)
        def _(p):
            peer = lax.rem(me + p, N)
            pltpu.make_async_remote_copy(
                src_ref=parts.at[chunk, peer % 2, :, pl.ds(pl.multiple_of(peer // 2 * OWN, 128), OWN)],
                dst_ref=landing.at[chunk, me],
                send_sem=send_sem.at[phase],
                recv_sem=recv_sem.at[phase, chunk],
                device_id={"tp": peer},
                device_id_type=pl.DeviceIdType.MESH,
            ).start()

    def spread_out(phase, chunk, whole):
        block = whole.at[chunk, my_half, :, my_columns]

        @pl.loop(1, N)
        def _(p):
            pltpu.make_async_remote_copy(
                src_ref=block,
                dst_ref=block,
                send_sem=send_sem.at[phase],
                recv_sem=recv_sem.at[phase, chunk],
                device_id={"tp": lax.rem(me + p, N)},
                device_id_type=pl.DeviceIdType.MESH,
            ).start()

    def arrived(phase, chunk):
        pltpu.make_async_copy(r1.at[0, pl.ds(0, N - 1)], r1.at[0, pl.ds(0, N - 1)], recv_sem.at[phase, chunk]).wait()

    def total_of(chunk, parts, landing):
        total = parts[chunk, my_half, :, my_columns].astype(F32)

        def add(p, total):
            return total + landing[chunk, lax.rem(me + p, N)].astype(F32)

        return lax.fori_loop(1, N, add, total, unroll=True)

    def project(chunk):
        rows = seen_v[pl.ds(chunk * PER, PER)].reshape(8 * PER, QD).astype(BF16)
        i, j = iota((CHUNK, 8 * PER), 0), iota((CHUNK, 8 * PER), 1)
        seen = dot(ones_where((j >> 3) * GROUP + (j & 3) == i), rows).astype(BF16)
        term = dot(seen, wo_v[...]).astype(BF16)
        p1[chunk, 0] = term[0:8]
        p1[chunk, 1] = term[8:16]
        scatter(0, chunk, p1, r1)

    def finish_h(chunk):
        arrived(0, chunk)
        x = x_v[chunk * 2 + my_half, :, my_columns].astype(F32)
        hb[chunk, my_half, :, my_columns] = (x + total_of(chunk, p1, r1)).astype(BF16)
        spread_out(1, chunk, hb)

    def mlp(chunk):
        arrived(1, chunk)
        h = hb[chunk].astype(F32).reshape(CHUNK, D)
        b = scaled(h, gain_m_ref[...].astype(F32))
        hidden = (jax.nn.silu(dot(b, wg_v[...])) * dot(b, wu_v[...])).astype(BF16)
        term = dot(hidden, wd_v[...]).astype(BF16)
        p2[chunk, 0] = term[0:8]
        p2[chunk, 1] = term[8:16]
        scatter(2, chunk, p2, r2)

    def finish_y(chunk):
        arrived(2, chunk)
        h = hb[chunk, my_half, :, my_columns].astype(F32)
        yb[chunk, my_half, :, my_columns] = (h + total_of(chunk, p2, r2)).astype(BF16)
        spread_out(3, chunk, yb)

    @pl.loop(0, GROUPS)
    def _(g):
        attend(g)
        chunk, at = g // PER, g % PER

        @pl.when(g == PER - 1)
        def _():
            for copy in late:
                copy.wait()
            pl.semaphore_wait(barrier, N - 1)

        @pl.when(at == PER - 1)
        def _():
            project(chunk)

            @pl.when(chunk >= 1)
            def _():
                mlp(chunk - 1)

        @pl.when((at == 1) & (chunk >= 1))
        def _():
            finish_h(chunk - 1)

            @pl.when(chunk >= 2)
            def _():
                finish_y(chunk - 2)

    last = CHUNKS - 1
    finish_h(last)
    finish_y(last - 1)
    mlp(last)
    finish_y(last)
    for chunk in range(CHUNKS):
        arrived(3, chunk)
    out = pltpu.make_async_copy(yb, y_hbm, out_sem)
    out.start()
    for phase in range(4):
        sent = r1.at[:, pl.ds(0, N - 1)]
        pltpu.make_async_copy(sent, sent, send_sem.at[phase]).wait()
    out.wait()


def turns():
    half = HEAD // 2
    angle = (SPAN - 1) * float(THETA) ** (-np.arange(half) / half)
    cos, sin = np.cos(angle), np.sin(angle)
    table = np.zeros((8, QD), np.float32)
    table[0] = np.tile(np.concatenate([cos, cos]), 2)
    table[1] = np.tile(np.concatenate([-sin, sin]), 2)
    return table


def solution(mesh):
    def step(x, k_cache, v_cache, gain_a, wq, wo, gain_m, w_gate, w_up, w_down):
        hbm = pl.BlockSpec(memory_space=pltpu.HBM)
        vmem = pl.BlockSpec(memory_space=pltpu.VMEM)

        def stacked(cache):
            return cache.transpose(0, 2, 3, 1).reshape(GROUPS, STACK, SPAN)

        y = pl.pallas_call(
            kernel,
            out_shape=jax.ShapeDtypeStruct((CHUNKS, 2, 8, D), BF16),
            in_specs=[hbm, hbm, hbm, vmem, vmem, hbm, hbm, vmem, hbm, hbm, hbm],
            out_specs=hbm,
            scratch_shapes=[
                pltpu.VMEM((ROWS // 8, 8, D), BF16),
                pltpu.VMEM((QD, D), BF16),
                pltpu.VMEM((QD, D), BF16),
                pltpu.VMEM((D, FF), BF16),
                pltpu.VMEM((D, FF), BF16),
                pltpu.VMEM((FF, D), BF16),
                pltpu.VMEM((SLOTS, STACK, SPAN), BF16),
                pltpu.VMEM((SLOTS, STACK, SPAN), BF16),
                pltpu.VMEM((GROUPS, 8, STACK), F32),
                pltpu.VMEM((8, SPAN), F32),
                pltpu.VMEM((8, SPAN), BF16),
                pltpu.VMEM((STACK, QD), BF16),
                pltpu.VMEM((GROUPS, 8, QD), F32),
                pltpu.VMEM((CHUNKS, 2, 8, D), BF16),
                pltpu.VMEM((CHUNKS, 2, 8, D), BF16),
                pltpu.VMEM((CHUNKS, N, 8, OWN), BF16),
                pltpu.VMEM((CHUNKS, N, 8, OWN), BF16),
                pltpu.VMEM((CHUNKS, 2, 8, D), BF16),
                pltpu.VMEM((CHUNKS, 2, 8, D), BF16),
                pltpu.SemaphoreType.DMA((SLOTS, PIECES)),
                pltpu.SemaphoreType.DMA((SLOTS, PIECES)),
                pltpu.SemaphoreType.DMA((6,)),
                pltpu.SemaphoreType.DMA((4,)),
                pltpu.SemaphoreType.DMA((4, CHUNKS)),
                pltpu.SemaphoreType.DMA,
            ],
            compiler_params=pltpu.CompilerParams(
                collective_id=0, has_side_effects=True, vmem_limit_bytes=60 * 2**20
            ),
            name="layer",
        )(
            x.reshape(ROWS // 8, 8, D), stacked(k_cache), stacked(v_cache), turns(), gain_a.reshape(1, D), wq.T, wo,
            gain_m.reshape(1, D), w_gate, w_up, w_down,
        )
        return y.reshape(ROWS, D)

    states, cache, columns, rows_of = P("dp", None), P("dp", None, "tp", None), P(None, "tp"), P("tp", None)
    return jax.shard_map(
        step,
        mesh=mesh,
        in_specs=(states, cache, cache, P(None), columns, rows_of, P(None), columns, columns, rows_of),
        out_specs=states,
        check_vma=False,
    )
```

```python
import functools

import jax
import jax.numpy as jnp
import numpy as np
from jax import lax
from jax.experimental import pallas as pl
from jax.experimental.pallas import tpu as pltpu
from jax.sharding import PartitionSpec as P

HEAD = 96
THETA = 10000

ROWS = 64
D = 3072
SPAN = 4096
QD = 192
FF = 512
GROUP = 4
GROUPS = ROWS // GROUP
STACK = GROUP * QD
SLOTS = 2
LAST_PIECES = 4
BLOCK = 8
BLOCKS = ROWS // BLOCK
BIG = 4
SMALL = 2
STEADY = GROUPS - 2 * SMALL
CHUNKS = STEADY // BIG + 2
N = 16
CHIPS = N // 2
OWN = D // CHIPS

F32, BF16 = jnp.float32, jnp.bfloat16
NT = (((1,), (1,)), ((), ()))
FAR_FIRST = (7, 6, 5, 3, 4, 2, 1)

def dot(a, b):
    return jnp.dot(a, b, preferred_element_type=F32)


def iota(shape, axis):
    return lax.broadcasted_iota(jnp.int32, shape, axis)


def ones_where(keep):
    return jnp.where(keep, 1.0, 0.0).astype(BF16)


def scaled(wide, gain):
    scale = lax.rsqrt(jnp.mean(wide * wide, -1, keepdims=True) + 1e-6)
    return (wide * scale * gain).astype(BF16)


def row_of(ref):
    gain = ref[...].astype(F32)
    return jnp.concatenate([gain[i : i + 1] for i in range(D // 128)], 1)


def any_of(d, values):
    found = d == values[0]
    for v in values[1:]:
        found = found | (d == v)
    return found


def kernel(
    x_hbm, k_hbm, v_hbm, turn_ref, gain_a_ref, wq_hbm, wo_hbm, gain_m_ref, wg_hbm, wu_hbm, wd_hbm,
    y_ref,
    x_v, wq_v, wo_v, wg_v, wu_v, wd_v, k_v, v_v, q_v, fold_v, seen_v,
    p1, p2, r1, r2, hb,
    k_sem, v_sem, w_sem, send_sem, recv_sem,
):
    me = lax.axis_index("tp")
    chip, core = me // 2, me % 2
    columns = pl.ds(pl.multiple_of(chip * OWN, 128), OWN)

    def chip_at(difference):
        return sum((chip // 2**b + (difference >> b)) % 2 * 2**b for b in range(3))

    chips = {difference: chip_at(difference) for difference in FAR_FIRST}

    def k_copy(g):
        slot = lax.rem(g, SLOTS)
        return pltpu.make_async_copy(k_hbm.at[g], k_v.at[slot], k_sem.at[slot])

    def v_copies(g, pieces):
        slot, width = lax.rem(g, SLOTS), SPAN // pieces
        spans = [pl.ds(i * width, width) for i in range(pieces)]
        return [
            (span, pltpu.make_async_copy(v_hbm.at[g, :, span], v_v.at[slot, :, span], v_sem.at[slot, i]))
            for i, span in enumerate(spans)
        ]

    early = [pltpu.make_async_copy(x_hbm, x_v, w_sem.at[0]), pltpu.make_async_copy(wq_hbm, wq_v, w_sem.at[1])]
    late = [
        pltpu.make_async_copy(wo_hbm, wo_v, w_sem.at[2]),
        pltpu.make_async_copy(wg_hbm, wg_v, w_sem.at[3]),
        pltpu.make_async_copy(wu_hbm, wu_v, w_sem.at[4]),
        pltpu.make_async_copy(wd_hbm, wd_v, w_sem.at[5]),
    ]
    for copy in early:
        copy.start()
    for g in range(SLOTS):
        k_copy(g).start()
        for _, copy in v_copies(g, 1):
            copy.start()
    for copy in late:
        copy.start()

    barrier = pltpu.get_barrier_semaphore()
    for p in range(1, N):
        pl.semaphore_signal(barrier, inc=1, device_id={"tp": lax.rem(me + p, N)}, device_id_type=pl.DeviceIdType.MESH)

    for copy in early:
        copy.wait()
    a = scaled(x_v[...].reshape(ROWS, D).astype(F32), row_of(gain_a_ref))
    q = lax.dot_general(a, wq_v[...], NT, preferred_element_type=F32).astype(BF16)
    i, j = iota((QD, QD), 0), iota((QD, QD), 1)
    first = (j < 48) | ((j >= 96) & (j < 144))
    swapped = dot(q, ones_where(((i - j == 48) & first) | ((i - j == -48) & ~first)))
    q = (q.astype(F32) * turn_ref[0:1, :] + swapped * turn_ref[1:2, :]).astype(BF16)
    places = [QD * n for n in range(GROUP)]
    spread = ones_where(any_of(iota((QD, STACK), 1) - iota((QD, STACK), 0), places))
    wide = dot(q, spread).astype(BF16)
    i = iota((2 * ROWS, ROWS), 0)
    wide = dot(ones_where((i >> 3) * GROUP + (i & 3) == iota((2 * ROWS, ROWS), 1)), wide)
    r, c = iota((2 * ROWS, STACK), 0), iota((2 * ROWS, STACK), 1)
    low = (r & 3) * QD + ((r >> 2) & 1) * HEAD
    q_v[...] = jnp.where((c >= low) & (c < low + HEAD), wide, 0.0).reshape(GROUPS, 8, STACK)
    fold_v[...] = ones_where(any_of(iota((STACK, QD), 0) - iota((STACK, QD), 1), places))

    def attend(g, pieces=1, refill=1):
        slot = lax.rem(g, SLOTS)
        k_copy(g).wait()
        s = dot(q_v[g].astype(BF16), k_v[slot]) * HEAD**-0.5
        if refill:
            k_copy(g + SLOTS).start()
        e = jnp.exp(s - jnp.max(s, -1, keepdims=True))
        weights = (e * (1.0 / jnp.sum(e, -1, keepdims=True))).astype(BF16)
        total = jnp.zeros((8, STACK), F32)
        for n, (span, copy) in enumerate(v_copies(g, pieces)):
            copy.wait()
            some = weights[:, n * SPAN // pieces : (n + 1) * SPAN // pieces]
            total += lax.dot_general(some, v_v[slot, :, span], NT, preferred_element_type=F32)
        if refill:
            for _, copy in v_copies(g + SLOTS, refill):
                copy.start()
        r, c = iota((8, STACK), 0), iota((8, STACK), 1)
        low = (r & 3) * QD + (r >> 2) * HEAD
        own = jnp.where((c >= low) & (c < low + HEAD), total, 0.0).astype(BF16)
        seen_v[g] = dot(own, fold_v[...])

    def send(phase, chunk, src, dst, peer):
        pltpu.make_async_remote_copy(
            src_ref=src,
            dst_ref=dst,
            send_sem=send_sem.at[phase],
            recv_sem=recv_sem.at[phase, chunk],
            device_id={"tp": peer},
            device_id_type=pl.DeviceIdType.MESH,
        ).start()

    def of(chunk):
        if isinstance(chunk, int) and chunk >= CHUNKS - 2:
            groups = SMALL
            first = STEADY + (chunk - (CHUNKS - 2)) * SMALL
        else:
            groups = BIG
            first = chunk * BIG
        blocks = groups * GROUP // BLOCK
        start = chunk * blocks if groups == BIG else first * GROUP // BLOCK
        return first, groups, blocks, pl.ds(start, blocks)

    def scatter(phase, chunk, parts, landing):
        rows = of(chunk)[3]
        for difference in FAR_FIRST:
            to = chips[difference]
            theirs = pl.ds(pl.multiple_of(to * OWN, 128), OWN)
            send(phase, chunk, parts.at[rows, :, theirs], landing.at[me, rows], to * 2 + 1)

        @pl.when(core == 0)
        def _():
            send(phase, chunk, parts.at[rows, :, columns], landing.at[me, rows], me + 1)

    def spread_out(phase, chunk, whole):
        block = whole.at[of(chunk)[3], :, columns]
        for difference in FAR_FIRST:
            send(phase, chunk, block, block, chips[difference] * 2)
            send(phase, chunk, block, block, chips[difference] * 2 + 1)
        send(phase, chunk, block, block, me - 1)

    def arrived(phase, chunk, count):
        some = r1.at[pl.ds(0, count), pl.ds(0, of(chunk)[2])]
        pltpu.make_async_copy(some, some, recv_sem.at[phase, chunk]).wait()

    def whole_arrived(phase, chunk):
        @pl.when(core == 1)
        def _():
            arrived(phase, chunk, CHIPS - 1)

        @pl.when(core == 0)
        def _():
            arrived(phase, chunk, CHIPS)

    def finish(phase, chunk, base, parts, landing, whole):
        rows = of(chunk)[3]

        @pl.when(core == 1)
        def _():
            arrived(phase, chunk, N - 1)
            total = parts[rows, :, columns].astype(F32)
            for p in range(1, N):
                total += landing[lax.rem(me + p, N), rows].astype(F32)
            whole[rows, :, columns] = (base[rows, :, columns].astype(F32) + total).astype(BF16)
            spread_out(phase + 1, chunk, whole)

    def project(chunk):
        first, groups, blocks, rows = of(chunk)
        both = seen_v[pl.ds(first, groups)].reshape(8 * groups, QD).astype(BF16)
        shape = (GROUP * groups, 8 * groups)
        i, j = iota(shape, 0), iota(shape, 1)
        seen = dot(ones_where((j >> 3) * GROUP + (j & 3) == i), both).astype(BF16)
        p1[rows] = dot(seen, wo_v[...]).reshape(blocks, BLOCK, D).astype(BF16)
        scatter(0, chunk, p1, r1)

    def finish_h(chunk):
        finish(0, chunk, x_v, p1, r1, hb)

    def mlp(chunk):
        _, _, blocks, rows = of(chunk)
        whole_arrived(1, chunk)
        b = scaled(hb[rows].astype(F32).reshape(blocks * BLOCK, D), row_of(gain_m_ref))
        hidden = (jax.nn.silu(dot(b, wg_v[...])) * dot(b, wu_v[...])).astype(BF16)
        p2[rows] = dot(hidden, wd_v[...]).reshape(blocks, BLOCK, D).astype(BF16)
        scatter(2, chunk, p2, r2)

    def finish_y(chunk):
        finish(2, chunk, hb, p2, r2, y_ref)

    @pl.loop(0, STEADY)
    def _(g):
        attend(g)
        chunk, at = g // BIG, g % BIG

        @pl.when(g == BIG - 1)
        def _():
            for copy in late:
                copy.wait()
            pl.semaphore_wait(barrier, N - 1)

        @pl.when(at == BIG - 1)
        def _():
            project(chunk)

            @pl.when(chunk >= 1)
            def _():
                mlp(chunk - 1)

        @pl.when((at == 1) & (chunk >= 1))
        def _():
            finish_h(chunk - 1)

            @pl.when(chunk >= 2)
            def _():
                finish_y(chunk - 2)

    attend(12)
    attend(13, refill=LAST_PIECES)
    project(3)
    finish_h(2)
    finish_y(1)
    attend(14, refill=0)
    mlp(2)
    finish_h(3)
    attend(15, pieces=LAST_PIECES, refill=0)
    project(4)
    mlp(3)
    finish_y(2)
    finish_h(4)
    finish_y(3)
    mlp(4)
    finish_y(4)
    for chunk in range(CHUNKS):
        whole_arrived(3, chunk)

    def sent(phase, count):
        some = r1.at[pl.ds(0, count)]
        pltpu.make_async_copy(some, some, send_sem.at[phase]).wait()

    @pl.when(core == 1)
    def _():
        for phase, count in ((0, CHIPS - 1), (1, N - 1), (2, CHIPS - 1), (3, N - 1)):
            sent(phase, count)

    @pl.when(core == 0)
    def _():
        for phase in (0, 2):
            sent(phase, CHIPS)


def turns():
    half = HEAD // 2
    angle = (SPAN - 1) * float(THETA) ** (-np.arange(half) / half)
    cos, sin = np.cos(angle), np.sin(angle)
    table = np.zeros((8, QD), np.float32)
    table[0] = np.tile(np.concatenate([cos, cos]), 2)
    table[1] = np.tile(np.concatenate([-sin, sin]), 2)
    return table


def solution(mesh):
    def step(x, k_cache, v_cache, gain_a, wq, wo, gain_m, w_gate, w_up, w_down):
        hbm = pl.BlockSpec(memory_space=pltpu.HBM)
        vmem = pl.BlockSpec(memory_space=pltpu.VMEM)

        def stacked(cache):
            return cache.transpose(0, 2, 3, 1).reshape(GROUPS, STACK, SPAN)

        y = pl.pallas_call(
            kernel,
            out_shape=pltpu.VMEM((BLOCKS, BLOCK, D), BF16),
            in_specs=[hbm, hbm, hbm, vmem, vmem, hbm, hbm, vmem, hbm, hbm, hbm],
            out_specs=vmem,
            scratch_shapes=[
                pltpu.VMEM((BLOCKS, BLOCK, D), BF16),
                pltpu.VMEM((QD, D), BF16),
                pltpu.VMEM((QD, D), BF16),
                pltpu.VMEM((D, FF), BF16),
                pltpu.VMEM((D, FF), BF16),
                pltpu.VMEM((FF, D), BF16),
                pltpu.VMEM((SLOTS, STACK, SPAN), BF16),
                pltpu.VMEM((SLOTS, STACK, SPAN), BF16),
                pltpu.VMEM((GROUPS, 8, STACK), F32),
                pltpu.VMEM((STACK, QD), BF16),
                pltpu.VMEM((GROUPS, 8, QD), F32),
                pltpu.VMEM((BLOCKS, BLOCK, D), BF16),
                pltpu.VMEM((BLOCKS, BLOCK, D), BF16),
                pltpu.VMEM((N, BLOCKS, BLOCK, OWN), BF16),
                pltpu.VMEM((N, BLOCKS, BLOCK, OWN), BF16),
                pltpu.VMEM((BLOCKS, BLOCK, D), BF16),
                pltpu.SemaphoreType.DMA((SLOTS,)),
                pltpu.SemaphoreType.DMA((SLOTS, LAST_PIECES)),
                pltpu.SemaphoreType.DMA((6,)),
                pltpu.SemaphoreType.DMA((4,)),
                pltpu.SemaphoreType.DMA((4, CHUNKS)),
            ],
            compiler_params=pltpu.CompilerParams(
                collective_id=0, has_side_effects=True, vmem_limit_bytes=60 * 2**20
            ),
            name="layer",
        )(
            x.reshape(BLOCKS, BLOCK, D), stacked(k_cache), stacked(v_cache), turns(), gain_a.reshape(D // 128, 128), wq.T, wo,
            gain_m.reshape(D // 128, 128), w_gate, w_up, w_down,
        )
        return y.reshape(ROWS, D)

    states, cache, columns, rows_of = P("dp", None), P("dp", None, "tp", None), P(None, "tp"), P("tp", None)
    return jax.shard_map(
        step,
        mesh=mesh,
        in_specs=(states, cache, cache, P(None), columns, rows_of, P(None), columns, columns, rows_of),
        out_specs=states,
        check_vma=False,
    )
```

```python
import functools

import jax
import jax.numpy as jnp
import numpy as np
from jax import lax
from jax.experimental import pallas as pl
from jax.experimental.pallas import tpu as pltpu
from jax.sharding import PartitionSpec as P

HEAD = 96
THETA = 10000

ROWS = 64
D = 3072
SPAN = 4096
QD = 192
FF = 512
GROUP = 4
GROUPS = ROWS // GROUP
STACK = GROUP * QD
SLOTS = 2
LAST_PIECES = 4
BLOCK = 8
BLOCKS = ROWS // BLOCK
BIG = 4
SMALL = 2
STEADY = GROUPS - 2 * SMALL
CHUNKS = STEADY // BIG + 2
N = 16
CHIPS = N // 2
OWN = D // CHIPS

F32, BF16 = jnp.float32, jnp.bfloat16
NT = (((1,), (1,)), ((), ()))
FAR_FIRST = (7, 6, 5, 3, 4, 2, 1)

def dot(a, b):
    return jnp.dot(a, b, preferred_element_type=F32)


def iota(shape, axis):
    return lax.broadcasted_iota(jnp.int32, shape, axis)


def ones_where(keep):
    return jnp.where(keep, 1.0, 0.0).astype(BF16)


def scaled(wide, gain):
    scale = lax.rsqrt(jnp.mean(wide * wide, -1, keepdims=True) + 1e-6)
    return (wide * scale * gain).astype(BF16)


def row_of(ref):
    gain = ref[...].astype(F32)
    return jnp.concatenate([gain[i : i + 1] for i in range(D // 128)], 1)


def any_of(d, values):
    found = d == values[0]
    for v in values[1:]:
        found = found | (d == v)
    return found


def kernel(
    x_hbm, k_hbm, v_hbm, turn_ref, gain_a_ref, wq_hbm, wo_hbm, gain_m_ref, wg_hbm, wu_hbm, wd_hbm,
    y_ref,
    x_v, wq_v, wo_v, wg_v, wu_v, wd_v, k_v, v_v, q_v, fold_v, seen_v,
    p1, p2, r1, r2, hb, weights_v, total_v,
    k_sem, v_sem, w_sem, send_sem, recv_sem,
):
    me = lax.axis_index("tp")
    chip, core = me // 2, me % 2
    columns = pl.ds(pl.multiple_of(chip * OWN, 128), OWN)

    def chip_at(difference):
        return sum((chip // 2**b + (difference >> b)) % 2 * 2**b for b in range(3))

    chips = {difference: chip_at(difference) for difference in FAR_FIRST}

    def copies(hbm, vmem, sems, g, pieces):
        slot, width = lax.rem(g, SLOTS), SPAN // pieces
        spans = [pl.ds(i * width, width) for i in range(pieces)]
        return [
            pltpu.make_async_copy(hbm.at[g, :, span], vmem.at[slot, :, span], sems.at[slot, i])
            for i, span in enumerate(spans)
        ]

    def k_copies(g, pieces=1):
        return copies(k_hbm, k_v, k_sem, g, pieces)

    def v_copies(g, pieces=1):
        return copies(v_hbm, v_v, v_sem, g, pieces)

    def start(some):
        for copy in some:
            copy.start()

    early = [pltpu.make_async_copy(x_hbm, x_v, w_sem.at[0]), pltpu.make_async_copy(wq_hbm, wq_v, w_sem.at[1])]
    late = [
        pltpu.make_async_copy(wo_hbm, wo_v, w_sem.at[2]),
        pltpu.make_async_copy(wg_hbm, wg_v, w_sem.at[3]),
        pltpu.make_async_copy(wu_hbm, wu_v, w_sem.at[4]),
        pltpu.make_async_copy(wd_hbm, wd_v, w_sem.at[5]),
    ]
    for copy in early:
        copy.start()
    for g in range(SLOTS):
        start(k_copies(g) + v_copies(g))
    for copy in late:
        copy.start()

    barrier = pltpu.get_barrier_semaphore()
    for p in range(1, N):
        pl.semaphore_signal(barrier, inc=1, device_id={"tp": lax.rem(me + p, N)}, device_id_type=pl.DeviceIdType.MESH)

    for copy in early:
        copy.wait()
    a = scaled(x_v[...].reshape(ROWS, D).astype(F32), row_of(gain_a_ref))
    q = lax.dot_general(a, wq_v[...], NT, preferred_element_type=F32).astype(BF16)
    i, j = iota((QD, QD), 0), iota((QD, QD), 1)
    first = (j < 48) | ((j >= 96) & (j < 144))
    swapped = dot(q, ones_where(((i - j == 48) & first) | ((i - j == -48) & ~first)))
    q = (q.astype(F32) * turn_ref[0:1, :] + swapped * turn_ref[1:2, :]).astype(BF16)
    places = [QD * n for n in range(GROUP)]
    spread = ones_where(any_of(iota((QD, STACK), 1) - iota((QD, STACK), 0), places))
    wide = dot(q, spread).astype(BF16)
    i = iota((2 * ROWS, ROWS), 0)
    wide = dot(ones_where((i >> 3) * GROUP + (i & 3) == iota((2 * ROWS, ROWS), 1)), wide)
    r, c = iota((2 * ROWS, STACK), 0), iota((2 * ROWS, STACK), 1)
    low = (r & 3) * QD + ((r >> 2) & 1) * HEAD
    q_v[...] = jnp.where((c >= low) & (c < low + HEAD), wide, 0.0).reshape(GROUPS, 8, STACK)
    fold_v[...] = ones_where(any_of(iota((STACK, QD), 0) - iota((STACK, QD), 1), places))

    def keep(g, total):
        r, c = iota((8, STACK), 0), iota((8, STACK), 1)
        low = (r & 3) * QD + (r >> 2) * HEAD
        own = jnp.where((c >= low) & (c < low + HEAD), total, 0.0).astype(BF16)
        seen_v[g] = dot(own, fold_v[...])

    def attend(g, pieces=1, after_keys=None, after_values=None):
        slot = lax.rem(g, SLOTS)

        @pl.when(me >= 0)
        def _():
            k_copies(g)[0].wait()
            s = dot(q_v[g].astype(BF16), k_v[slot]) * HEAD**-0.5
            if after_keys:
                after_keys()
            e = jnp.exp(s - jnp.max(s, -1, keepdims=True))
            weights_v[...] = (e * (1.0 / jnp.sum(e, -1, keepdims=True))).astype(BF16)

        for n, copy in enumerate(v_copies(g, pieces)):

            @pl.when(me >= 0)
            def _():
                copy.wait()
                some = pl.ds(n * SPAN // pieces, SPAN // pieces)
                total = lax.dot_general(weights_v[:, some], v_v[slot, :, some], NT, preferred_element_type=F32)
                if n:
                    total += total_v[...]
                if n == pieces - 1:
                    keep(g, total)
                else:
                    total_v[...] = total

        if after_values:
            after_values()

    def send(phase, chunk, src, dst, peer):
        pltpu.make_async_remote_copy(
            src_ref=src,
            dst_ref=dst,
            send_sem=send_sem.at[phase],
            recv_sem=recv_sem.at[phase, chunk],
            device_id={"tp": peer},
            device_id_type=pl.DeviceIdType.MESH,
        ).start()

    def of(chunk):
        if isinstance(chunk, int) and chunk >= CHUNKS - 2:
            groups = SMALL
            first = STEADY + (chunk - (CHUNKS - 2)) * SMALL
        else:
            groups = BIG
            first = chunk * BIG
        blocks = groups * GROUP // BLOCK
        start = chunk * blocks if groups == BIG else first * GROUP // BLOCK
        return first, groups, blocks, pl.ds(start, blocks)

    def scatter(phase, chunk, parts, landing):
        rows = of(chunk)[3]
        for difference in FAR_FIRST:
            to = chips[difference]
            theirs = pl.ds(pl.multiple_of(to * OWN, 128), OWN)
            send(phase, chunk, parts.at[rows, :, theirs], landing.at[me, rows], to * 2 + 1)

        @pl.when(core == 0)
        def _():
            send(phase, chunk, parts.at[rows, :, columns], landing.at[me, rows], me + 1)

    def spread_out(phase, chunk, whole):
        block = whole.at[of(chunk)[3], :, columns]
        for difference in FAR_FIRST:
            send(phase, chunk, block, block, chips[difference] * 2)
            send(phase, chunk, block, block, chips[difference] * 2 + 1)
        send(phase, chunk, block, block, me - 1)

    def arrived(phase, chunk, count):
        some = r1.at[pl.ds(0, count), pl.ds(0, of(chunk)[2])]
        pltpu.make_async_copy(some, some, recv_sem.at[phase, chunk]).wait()

    def whole_arrived(phase, chunk):
        @pl.when(core == 1)
        def _():
            arrived(phase, chunk, CHIPS - 1)

        @pl.when(core == 0)
        def _():
            arrived(phase, chunk, CHIPS)

    def finish(phase, chunk, base, parts, landing, whole):
        rows = of(chunk)[3]

        @pl.when(core == 1)
        def _():
            arrived(phase, chunk, N - 1)
            total = parts[rows, :, columns].astype(F32)
            for p in range(1, N):
                total += landing[lax.rem(me + p, N), rows].astype(F32)
            whole[rows, :, columns] = (base[rows, :, columns].astype(F32) + total).astype(BF16)
            spread_out(phase + 1, chunk, whole)

    def project(chunk):
        first, groups, blocks, rows = of(chunk)
        both = seen_v[pl.ds(first, groups)].reshape(8 * groups, QD).astype(BF16)
        shape = (GROUP * groups, 8 * groups)
        i, j = iota(shape, 0), iota(shape, 1)
        seen = dot(ones_where((j >> 3) * GROUP + (j & 3) == i), both).astype(BF16)
        p1[rows] = dot(seen, wo_v[...]).reshape(blocks, BLOCK, D).astype(BF16)
        scatter(0, chunk, p1, r1)

    def finish_h(chunk):
        finish(0, chunk, x_v, p1, r1, hb)

    def mlp(chunk):
        _, _, blocks, rows = of(chunk)
        whole_arrived(1, chunk)
        b = scaled(hb[rows].astype(F32).reshape(blocks * BLOCK, D), row_of(gain_m_ref))
        hidden = (jax.nn.silu(dot(b, wg_v[...])) * dot(b, wu_v[...])).astype(BF16)
        p2[rows] = dot(hidden, wd_v[...]).reshape(blocks, BLOCK, D).astype(BF16)
        scatter(2, chunk, p2, r2)

    def finish_y(chunk):
        finish(2, chunk, hb, p2, r2, y_ref)

    @pl.loop(0, STEADY)
    def _(g):
        attend(g, after_keys=lambda: start(k_copies(g + SLOTS)), after_values=lambda: start(v_copies(g + SLOTS)))
        chunk, at = g // BIG, g % BIG

        @pl.when(g == BIG - 1)
        def _():
            for copy in late:
                copy.wait()
            pl.semaphore_wait(barrier, N - 1)

        @pl.when(at == BIG - 1)
        def _():
            project(chunk)

            @pl.when(chunk >= 1)
            def _():
                mlp(chunk - 1)

        @pl.when((at == 1) & (chunk >= 1))
        def _():
            finish_h(chunk - 1)

            @pl.when(chunk >= 2)
            def _():
                finish_y(chunk - 2)

    attend(12, after_keys=lambda: start(k_copies(14)), after_values=lambda: start(v_copies(14, 1)))
    attend(13, after_keys=lambda: start(k_copies(15)), after_values=lambda: start(v_copies(15, LAST_PIECES)[0:1]))
    project(3)
    finish_h(2)
    attend(14, after_keys=lambda: start(v_copies(15, LAST_PIECES)[1:2] + v_copies(15, LAST_PIECES)[2:3]), after_values=lambda: start(v_copies(15, LAST_PIECES)[3:4]))
    attend(15, pieces=LAST_PIECES)
    project(4)
    finish_h(3)
    mlp(2)
    finish_h(4)
    finish_y(1)
    mlp(3)
    mlp(4)
    finish_y(2)
    finish_y(3)
    finish_y(4)
    for chunk in range(CHUNKS):
        whole_arrived(3, chunk)

    def sent(phase, count):
        some = r1.at[pl.ds(0, count)]
        pltpu.make_async_copy(some, some, send_sem.at[phase]).wait()

    @pl.when(core == 1)
    def _():
        for phase, count in ((0, CHIPS - 1), (1, N - 1), (2, CHIPS - 1), (3, N - 1)):
            sent(phase, count)

    @pl.when(core == 0)
    def _():
        for phase in (0, 2):
            sent(phase, CHIPS)


def turns():
    half = HEAD // 2
    angle = (SPAN - 1) * float(THETA) ** (-np.arange(half) / half)
    cos, sin = np.cos(angle), np.sin(angle)
    table = np.zeros((8, QD), np.float32)
    table[0] = np.tile(np.concatenate([cos, cos]), 2)
    table[1] = np.tile(np.concatenate([-sin, sin]), 2)
    return table


def solution(mesh):
    def step(x, k_cache, v_cache, gain_a, wq, wo, gain_m, w_gate, w_up, w_down):
        hbm = pl.BlockSpec(memory_space=pltpu.HBM)
        vmem = pl.BlockSpec(memory_space=pltpu.VMEM)

        def stacked(cache):
            return cache.transpose(0, 2, 3, 1).reshape(GROUPS, STACK, SPAN)

        y = pl.pallas_call(
            kernel,
            out_shape=pltpu.VMEM((BLOCKS, BLOCK, D), BF16),
            in_specs=[hbm, hbm, hbm, vmem, vmem, hbm, hbm, vmem, hbm, hbm, hbm],
            out_specs=vmem,
            scratch_shapes=[
                pltpu.VMEM((BLOCKS, BLOCK, D), BF16),
                pltpu.VMEM((QD, D), BF16),
                pltpu.VMEM((QD, D), BF16),
                pltpu.VMEM((D, FF), BF16),
                pltpu.VMEM((D, FF), BF16),
                pltpu.VMEM((FF, D), BF16),
                pltpu.VMEM((SLOTS, STACK, SPAN), BF16),
                pltpu.VMEM((SLOTS, STACK, SPAN), BF16),
                pltpu.VMEM((GROUPS, 8, STACK), F32),
                pltpu.VMEM((STACK, QD), BF16),
                pltpu.VMEM((GROUPS, 8, QD), F32),
                pltpu.VMEM((BLOCKS, BLOCK, D), BF16),
                pltpu.VMEM((BLOCKS, BLOCK, D), BF16),
                pltpu.VMEM((N, BLOCKS, BLOCK, OWN), BF16),
                pltpu.VMEM((N, BLOCKS, BLOCK, OWN), BF16),
                pltpu.VMEM((BLOCKS, BLOCK, D), BF16),
                pltpu.VMEM((8, SPAN), BF16),
                pltpu.VMEM((8, STACK), F32),
                pltpu.SemaphoreType.DMA((SLOTS, LAST_PIECES)),
                pltpu.SemaphoreType.DMA((SLOTS, LAST_PIECES)),
                pltpu.SemaphoreType.DMA((6,)),
                pltpu.SemaphoreType.DMA((4,)),
                pltpu.SemaphoreType.DMA((4, CHUNKS)),
            ],
            compiler_params=pltpu.CompilerParams(
                collective_id=0, has_side_effects=True, vmem_limit_bytes=60 * 2**20
            ),
            name="layer",
        )(
            x.reshape(BLOCKS, BLOCK, D), stacked(k_cache), stacked(v_cache), turns(), gain_a.reshape(D // 128, 128), wq.T, wo,
            gain_m.reshape(D // 128, 128), w_gate, w_up, w_down,
        )
        return y.reshape(ROWS, D)

    states, cache, columns, rows_of = P("dp", None), P("dp", None, "tp", None), P(None, "tp"), P("tp", None)
    return jax.shard_map(
        step,
        mesh=mesh,
        in_specs=(states, cache, cache, P(None), columns, rows_of, P(None), columns, columns, rows_of),
        out_specs=states,
        check_vma=False,
    )
```

```python
import functools

import jax
import jax.numpy as jnp
import numpy as np
from jax import lax
from jax.experimental import pallas as pl
from jax.experimental.pallas import tpu as pltpu
from jax.sharding import PartitionSpec as P

HEAD = 96
THETA = 10000

ROWS = 64
D = 3072
SPAN = 4096
QD = 192
FF = 512
GROUP = 4
GROUPS = ROWS // GROUP
STACK = GROUP * QD
SLOTS = 2
LAST_PIECES = 2
BLOCK = 8
BLOCKS = ROWS // BLOCK
BIG = 4
SMALL = 2
STEADY = GROUPS - 2 * SMALL
CHUNKS = STEADY // BIG + 2
N = 16
CHIPS = N // 2
OWN = D // CHIPS

F32, BF16 = jnp.float32, jnp.bfloat16
NT = (((1,), (1,)), ((), ()))
FAR_FIRST = (7, 6, 5, 3, 4, 2, 1)

def dot(a, b):
    return jnp.dot(a, b, preferred_element_type=F32)


def iota(shape, axis):
    return lax.broadcasted_iota(jnp.int32, shape, axis)


def ones_where(keep):
    return jnp.where(keep, 1.0, 0.0).astype(BF16)


def scaled(wide, gain):
    scale = lax.rsqrt(jnp.mean(wide * wide, -1, keepdims=True) + 1e-6)
    return (wide * scale * gain).astype(BF16)


def row_of(ref):
    gain = ref[...].astype(F32)
    return jnp.concatenate([gain[i : i + 1] for i in range(D // 128)], 1)


def any_of(d, values):
    found = d == values[0]
    for v in values[1:]:
        found = found | (d == v)
    return found


def kernel(
    x_hbm, k_hbm, v_hbm, turn_ref, gain_a_ref, wq_hbm, wo_hbm, gain_m_ref, wg_hbm, wu_hbm, wd_hbm,
    y_ref,
    x_v, wq_v, wo_v, wg_v, wu_v, wd_v, k_v, v_v, q_v, fold_v, seen_v,
    p1, p2, r1, r2, hb, weights_v, total_v,
    k_sem, v_sem, w_sem, send_sem, recv_sem,
):
    me = lax.axis_index("tp")
    chip, core = me // 2, me % 2
    columns = pl.ds(pl.multiple_of(chip * OWN, 128), OWN)

    def chip_at(difference):
        return sum((chip // 2**b + (difference >> b)) % 2 * 2**b for b in range(3))

    chips = {difference: chip_at(difference) for difference in FAR_FIRST}

    def copies(hbm, vmem, sems, g, pieces):
        slot, width = lax.rem(g, SLOTS), SPAN // pieces
        spans = [pl.ds(i * width, width) for i in range(pieces)]
        return [
            pltpu.make_async_copy(hbm.at[g, :, span], vmem.at[slot, :, span], sems.at[slot, i])
            for i, span in enumerate(spans)
        ]

    def k_copies(g, pieces=1):
        return copies(k_hbm, k_v, k_sem, g, pieces)

    def v_copies(g, pieces=1):
        return copies(v_hbm, v_v, v_sem, g, pieces)

    def start(some):
        for copy in some:
            copy.start()

    early = [pltpu.make_async_copy(x_hbm, x_v, w_sem.at[0]), pltpu.make_async_copy(wq_hbm, wq_v, w_sem.at[1])]
    late = [
        pltpu.make_async_copy(wo_hbm, wo_v, w_sem.at[2]),
        pltpu.make_async_copy(wg_hbm, wg_v, w_sem.at[3]),
        pltpu.make_async_copy(wu_hbm, wu_v, w_sem.at[4]),
        pltpu.make_async_copy(wd_hbm, wd_v, w_sem.at[5]),
    ]
    for copy in early:
        copy.start()
    for g in range(SLOTS):
        start(k_copies(g) + v_copies(g))
    for copy in late:
        copy.start()

    barrier = pltpu.get_barrier_semaphore()
    for p in range(1, N):
        pl.semaphore_signal(barrier, inc=1, device_id={"tp": lax.rem(me + p, N)}, device_id_type=pl.DeviceIdType.MESH)

    for copy in early:
        copy.wait()
    a = scaled(x_v[...].reshape(ROWS, D).astype(F32), row_of(gain_a_ref))
    q = lax.dot_general(a, wq_v[...], NT, preferred_element_type=F32).astype(BF16)
    i, j = iota((QD, QD), 0), iota((QD, QD), 1)
    first = (j < 48) | ((j >= 96) & (j < 144))
    swapped = dot(q, ones_where(((i - j == 48) & first) | ((i - j == -48) & ~first)))
    q = (q.astype(F32) * turn_ref[0:1, :] + swapped * turn_ref[1:2, :]).astype(BF16)
    places = [QD * n for n in range(GROUP)]
    spread = ones_where(any_of(iota((QD, STACK), 1) - iota((QD, STACK), 0), places))
    wide = dot(q, spread).astype(BF16)
    i = iota((2 * ROWS, ROWS), 0)
    wide = dot(ones_where((i >> 3) * GROUP + (i & 3) == iota((2 * ROWS, ROWS), 1)), wide)
    r, c = iota((2 * ROWS, STACK), 0), iota((2 * ROWS, STACK), 1)
    low = (r & 3) * QD + ((r >> 2) & 1) * HEAD
    q_v[...] = jnp.where((c >= low) & (c < low + HEAD), wide, 0.0).reshape(GROUPS, 8, STACK)
    fold_v[...] = ones_where(any_of(iota((STACK, QD), 0) - iota((STACK, QD), 1), places))

    def keep(g, total):
        r, c = iota((8, STACK), 0), iota((8, STACK), 1)
        low = (r & 3) * QD + (r >> 2) * HEAD
        own = jnp.where((c >= low) & (c < low + HEAD), total, 0.0).astype(BF16)
        seen_v[g] = dot(own, fold_v[...])

    def attend(g, pieces=1, after_keys=None, after_values=None):
        slot = lax.rem(g, SLOTS)

        @pl.when(me >= 0)
        def _():
            k_copies(g)[0].wait()
            s = dot(q_v[g].astype(BF16), k_v[slot]) * HEAD**-0.5
            if after_keys:
                after_keys()
            e = jnp.exp(s - jnp.max(s, -1, keepdims=True))
            weights_v[...] = (e * (1.0 / jnp.sum(e, -1, keepdims=True))).astype(BF16)

        for n, copy in enumerate(v_copies(g, pieces)):

            @pl.when(me >= 0)
            def _():
                copy.wait()
                some = pl.ds(n * SPAN // pieces, SPAN // pieces)
                total = lax.dot_general(weights_v[:, some], v_v[slot, :, some], NT, preferred_element_type=F32)
                if n:
                    total += total_v[...]
                if n == pieces - 1:
                    keep(g, total)
                else:
                    total_v[...] = total

        if after_values:
            after_values()

    def send(phase, chunk, src, dst, peer):
        pltpu.make_async_remote_copy(
            src_ref=src,
            dst_ref=dst,
            send_sem=send_sem.at[phase],
            recv_sem=recv_sem.at[phase, chunk],
            device_id={"tp": peer},
            device_id_type=pl.DeviceIdType.MESH,
        ).start()

    def of(chunk):
        if isinstance(chunk, int) and chunk >= CHUNKS - 2:
            groups = SMALL
            first = STEADY + (chunk - (CHUNKS - 2)) * SMALL
        else:
            groups = BIG
            first = chunk * BIG
        blocks = groups * GROUP // BLOCK
        start = chunk * blocks if groups == BIG else first * GROUP // BLOCK
        return first, groups, blocks, pl.ds(start, blocks)

    def scatter(phase, chunk, parts, landing):
        rows = of(chunk)[3]
        for difference in FAR_FIRST:
            to = chips[difference]
            theirs = pl.ds(pl.multiple_of(to * OWN, 128), OWN)
            send(phase, chunk, parts.at[rows, :, theirs], landing.at[me, rows], to * 2 + 1)

        @pl.when(core == 0)
        def _():
            send(phase, chunk, parts.at[rows, :, columns], landing.at[me, rows], me + 1)

    def spread_out(phase, chunk, whole):
        block = whole.at[of(chunk)[3], :, columns]
        for to in (0, 1):
            for difference in FAR_FIRST:
                send(phase, chunk, block, block, chips[difference] * 2 + to)
        send(phase, chunk, block, block, me - 1)

    def arrived(phase, chunk, count):
        some = r1.at[pl.ds(0, count), pl.ds(0, of(chunk)[2])]
        pltpu.make_async_copy(some, some, recv_sem.at[phase, chunk]).wait()

    def whole_arrived(phase, chunk):
        @pl.when(core == 1)
        def _():
            arrived(phase, chunk, CHIPS - 1)

        @pl.when(core == 0)
        def _():
            arrived(phase, chunk, CHIPS)

    def finish(phase, chunk, base, parts, landing, whole):
        rows = of(chunk)[3]

        @pl.when(core == 1)
        def _():
            arrived(phase, chunk, N - 1)
            total = parts[rows, :, columns].astype(F32)
            for p in range(1, N):
                total += landing[lax.rem(me + p, N), rows].astype(F32)
            whole[rows, :, columns] = (base[rows, :, columns].astype(F32) + total).astype(BF16)
            spread_out(phase + 1, chunk, whole)

    def project(chunk):
        first, groups, blocks, rows = of(chunk)
        both = seen_v[pl.ds(first, groups)].reshape(8 * groups, QD).astype(BF16)
        shape = (GROUP * groups, 8 * groups)
        i, j = iota(shape, 0), iota(shape, 1)
        seen = dot(ones_where((j >> 3) * GROUP + (j & 3) == i), both).astype(BF16)
        p1[rows] = dot(seen, wo_v[...]).reshape(blocks, BLOCK, D).astype(BF16)
        scatter(0, chunk, p1, r1)

    def finish_h(chunk):
        finish(0, chunk, x_v, p1, r1, hb)

    def mlp(chunk):
        _, _, blocks, rows = of(chunk)
        whole_arrived(1, chunk)
        b = scaled(hb[rows].astype(F32).reshape(blocks * BLOCK, D), row_of(gain_m_ref))
        hidden = (jax.nn.silu(dot(b, wg_v[...])) * dot(b, wu_v[...])).astype(BF16)
        p2[rows] = dot(hidden, wd_v[...]).reshape(blocks, BLOCK, D).astype(BF16)
        scatter(2, chunk, p2, r2)

    def finish_y(chunk):
        finish(2, chunk, hb, p2, r2, y_ref)

    @pl.loop(0, STEADY)
    def _(g):
        attend(g, after_keys=lambda: start(k_copies(g + SLOTS)), after_values=lambda: start(v_copies(g + SLOTS)))
        chunk, at = g // BIG, g % BIG

        @pl.when(g == BIG - 1)
        def _():
            for copy in late:
                copy.wait()
            pl.semaphore_wait(barrier, N - 1)

        @pl.when(at == BIG - 1)
        def _():
            project(chunk)

            @pl.when(chunk >= 1)
            def _():
                mlp(chunk - 1)

        @pl.when((at == 1) & (chunk >= 1))
        def _():
            finish_h(chunk - 1)

            @pl.when(chunk >= 2)
            def _():
                finish_y(chunk - 2)

    attend(12, after_keys=lambda: start(k_copies(14)), after_values=lambda: start(v_copies(14, 1)))
    attend(13, after_keys=lambda: start(k_copies(15)), after_values=lambda: start(v_copies(15, LAST_PIECES)[0:1]))
    project(3)
    finish_h(2)
    attend(14, after_values=lambda: start(v_copies(15, LAST_PIECES)[1:2]))
    attend(15, pieces=LAST_PIECES)
    project(4)
    finish_h(3)
    mlp(2)
    finish_h(4)
    finish_y(1)
    mlp(3)
    mlp(4)
    finish_y(2)
    finish_y(3)
    finish_y(4)
    for chunk in range(CHUNKS):
        whole_arrived(3, chunk)

    def sent(phase, count):
        some = r1.at[pl.ds(0, count)]
        pltpu.make_async_copy(some, some, send_sem.at[phase]).wait()

    @pl.when(core == 1)
    def _():
        for phase, count in ((0, CHIPS - 1), (1, N - 1), (2, CHIPS - 1), (3, N - 1)):
            sent(phase, count)

    @pl.when(core == 0)
    def _():
        for phase in (0, 2):
            sent(phase, CHIPS)


def turns():
    half = HEAD // 2
    angle = (SPAN - 1) * float(THETA) ** (-np.arange(half) / half)
    cos, sin = np.cos(angle), np.sin(angle)
    table = np.zeros((8, QD), np.float32)
    table[0] = np.tile(np.concatenate([cos, cos]), 2)
    table[1] = np.tile(np.concatenate([-sin, sin]), 2)
    return table


def solution(mesh):
    def step(x, k_cache, v_cache, gain_a, wq, wo, gain_m, w_gate, w_up, w_down):
        hbm = pl.BlockSpec(memory_space=pltpu.HBM)
        vmem = pl.BlockSpec(memory_space=pltpu.VMEM)

        def stacked(cache):
            return cache.transpose(0, 2, 3, 1).reshape(GROUPS, STACK, SPAN)

        y = pl.pallas_call(
            kernel,
            out_shape=pltpu.VMEM((BLOCKS, BLOCK, D), BF16),
            in_specs=[hbm, hbm, hbm, vmem, vmem, hbm, hbm, vmem, hbm, hbm, hbm],
            out_specs=vmem,
            scratch_shapes=[
                pltpu.VMEM((BLOCKS, BLOCK, D), BF16),
                pltpu.VMEM((QD, D), BF16),
                pltpu.VMEM((QD, D), BF16),
                pltpu.VMEM((D, FF), BF16),
                pltpu.VMEM((D, FF), BF16),
                pltpu.VMEM((FF, D), BF16),
                pltpu.VMEM((SLOTS, STACK, SPAN), BF16),
                pltpu.VMEM((SLOTS, STACK, SPAN), BF16),
                pltpu.VMEM((GROUPS, 8, STACK), F32),
                pltpu.VMEM((STACK, QD), BF16),
                pltpu.VMEM((GROUPS, 8, QD), F32),
                pltpu.VMEM((BLOCKS, BLOCK, D), BF16),
                pltpu.VMEM((BLOCKS, BLOCK, D), BF16),
                pltpu.VMEM((N, BLOCKS, BLOCK, OWN), BF16),
                pltpu.VMEM((N, BLOCKS, BLOCK, OWN), BF16),
                pltpu.VMEM((BLOCKS, BLOCK, D), BF16),
                pltpu.VMEM((8, SPAN), BF16),
                pltpu.VMEM((8, STACK), F32),
                pltpu.SemaphoreType.DMA((SLOTS, LAST_PIECES)),
                pltpu.SemaphoreType.DMA((SLOTS, LAST_PIECES)),
                pltpu.SemaphoreType.DMA((6,)),
                pltpu.SemaphoreType.DMA((4,)),
                pltpu.SemaphoreType.DMA((4, CHUNKS)),
            ],
            compiler_params=pltpu.CompilerParams(
                collective_id=0, has_side_effects=True, vmem_limit_bytes=60 * 2**20
            ),
            name="layer",
        )(
            x.reshape(BLOCKS, BLOCK, D), stacked(k_cache), stacked(v_cache), turns(), gain_a.reshape(D // 128, 128), wq.T, wo,
            gain_m.reshape(D // 128, 128), w_gate, w_up, w_down,
        )
        return y.reshape(ROWS, D)

    states, cache, columns, rows_of = P("dp", None), P("dp", None, "tp", None), P(None, "tp"), P("tp", None)
    return jax.shard_map(
        step,
        mesh=mesh,
        in_specs=(states, cache, cache, P(None), columns, rows_of, P(None), columns, columns, rows_of),
        out_specs=states,
        check_vma=False,
    )
```
